256 devices in a mesh: groups: 4 (over y, x), dp: 2 (over core), seq: 32 (over z).
Axes of the slice: x: 2, y: 2, z: 32, core: 2. Of those that a mesh axis runs over, the one named last changes fastest.
The devices are a block of a 4x8x32 slice.
Arguments:
- history: bfloat16 [16, 3072, 1024], P(('groups', 'dp'), 'seq'), parts along dimension 0, may hold values from -20 to 20
- candidates: bfloat16 [8, 2048, 1024], P(('groups', 'dp'), 'seq'), parts along dimension 0, may hold values from -6 to 6
- lengths: int32 [16], P(('groups', 'dp')), parts along dimension 0, may hold values from 384 to 3072
- assignment: int32 [8, 2048], P(('groups', 'dp'), 'seq'), parts along dimension 0, may hold values from 0 to 1, as said below
- weight_in: bfloat16 [1024, 4096], replicated, may hold values from -0.1875 to 0.1875
- weight_out: bfloat16 [1024, 1024], replicated, may hold values from -0.1875 to 0.1875
- gain_in: float32 [1024], replicated, may hold values from 0.25 to 1.75
- gain_attn: float32 [1024], replicated, may hold values from 0.25 to 1.75
Outputs:
- history_out: bfloat16 [16, 3072, 1024], P(('groups', 'dp'), 'seq'), parts along dimension 0
- candidate_out: bfloat16 [8, 2048, 1024], P(('groups', 'dp'), 'seq'), parts along dimension 0
The draws below stay inside these ranges and needn't reach their ends.
There are 4 independent parts, one for each index of `groups`. The reference program is written for one: setup_inputs(seed, part) draws one part's arguments, and reference() takes and returns one part's arrays. A program takes and returns all parts, laid end to end along the dimension named above; an argument that names none is the same for every part. Nothing has to cross between parts.
Inputs may be any that keep to these rules, and one draw needn't show every extreme that they name: `assignment`: of the 64 candidates of one device, at most 40 belong to either history; in every dp index some device has exactly 40 of the first and another exactly 40 of the second.
All inputs are finite; a program needn't handle non-finite values.
Results may differ from the reference program's by a relative error of at most 0.0075.
Values may be sent and summed in bfloat16 or wider, within the bound.
A program may use at most 192 MiB of HBM per device.

```python
import math
import jax
import jax.numpy as jnp
from jax import lax

D = 1024
H = 16
HD = 64
HIST_DP = 2
CAND_DEV = 64
LENGTH = 3072
CAP = 40
HISTS = 4
CS = 2048
N_DP = 2
N_SEQ = 32


def draw_history(key, part):
    first_key = jax.random.fold_in(key, 11)
    base = jnp.clip(jax.random.normal(first_key, (HISTS, LENGTH, D), jnp.float32), -4.0, 4.0)
    return base.astype(jnp.bfloat16)


def draw_assignment(key, part):
    count_key = jax.random.fold_in(key, 21)
    full_key = jax.random.fold_in(key, 22)
    other_key = jax.random.fold_in(key, 23)
    order_key = jax.random.fold_in(key, 24)
    counts = jax.random.randint(count_key, (N_DP, N_SEQ), CAND_DEV - CAP, CAP + 1)
    full_block = jax.random.randint(full_key, (N_DP, 1), 0, N_SEQ)
    other_block = (full_block + 1 + jax.random.randint(other_key, (N_DP, 1), 0, N_SEQ - 1)) % N_SEQ
    blocks = jnp.arange(N_SEQ, dtype=jnp.int32)[None, :]
    counts = jnp.where(blocks == full_block, CAP, counts)
    counts = jnp.where(blocks == other_block, CAND_DEV - CAP, counts)
    row_keys = jax.random.split(order_key, N_DP * N_SEQ)
    ranks = jax.vmap(lambda one_key: jax.random.permutation(one_key, jnp.arange(CAND_DEV, dtype=jnp.int32)))(row_keys)
    ranks = ranks.reshape(N_DP, N_SEQ, CAND_DEV)
    chosen = (ranks >= counts[:, :, None]).astype(jnp.int32)
    return chosen.reshape(N_DP, CS)


def touch_ends(array, own_key, low, top_value):
    place = [jax.random.randint(jax.random.fold_in(own_key, axis), (), 0, length) for axis, length in enumerate(array.shape)]
    main_axis = array.shape.index(max(array.shape))
    neighbour = place[:main_axis] + [(place[main_axis] + 1) % array.shape[main_axis]] + place[main_axis + 1:]
    return array.at[tuple(place)].set(low).at[tuple(neighbour)].set(top_value)


def block_levels(rng, dims, pieces, low, largest):
    level = 1.0
    for dim, blocks in pieces:
        heights = jax.random.uniform(jax.random.fold_in(jax.random.fold_in(rng, 6), dim), (blocks,), jnp.float32, low / len(pieces), largest / len(pieces))
        level = level * jnp.repeat(jnp.exp(heights), dims[dim] // blocks).reshape((-1,) + (1,) * (len(dims) - 1 - dim))
    return level


def normal_values(own_key, dims, width, limit, cuts=(), kind=jnp.bfloat16):
    entries = jax.random.normal(own_key, dims, jnp.float32) * width
    if len(cuts) > 0:
        entries = block_levels(own_key, dims, cuts, -0.22, 0.18) * entries
    return jnp.clip(entries, min=-limit, max=limit).astype(kind)


def setup_inputs(seed: int = 0, part: int = 0) -> dict:
    seeds = jax.random.split(jax.random.key(seed), 9)
    part_splits = jax.random.split(jax.random.fold_in(seeds[8], part), 9)
    history = draw_history(jax.random.fold_in(jax.random.fold_in(seeds[8], part), 71), part)
    candidates = normal_values(part_splits[1], (N_DP, CS, D), 1.0, 6.0, ((0, 2), (1, 32)))
    lengths = touch_ends(jax.random.randint(part_splits[2], (HISTS,), LENGTH // 8, LENGTH + 1), jax.random.fold_in(part_splits[2], 1), LENGTH // 8, LENGTH).astype(jnp.int32)
    assignment = draw_assignment(jax.random.fold_in(jax.random.fold_in(seeds[8], part), 71), part)
    weight_in = normal_values(seeds[4], (D, 4 * D), D ** -0.5, 0.1875)
    weight_out = normal_values(seeds[5], (D, D), D ** -0.5, 0.1875)
    gain_in = jnp.clip(1.0 + 0.15 * jax.random.normal(seeds[6], (D,), jnp.float32), 0.25, 1.75)
    gain_attn = jnp.clip(1.0 + 0.15 * jax.random.normal(seeds[7], (D,), jnp.float32), 0.25, 1.75)
    return {"history": history, "candidates": candidates, "lengths": lengths, "assignment": assignment, "weight_in": weight_in, "weight_out": weight_out, "gain_in": gain_in, "gain_attn": gain_attn}


def rms_apply(values, gain):
    return values * lax.rsqrt(lax.optimization_barrier(jnp.mean(values * values, axis=-1, keepdims=True)) + 1e-06) * gain

def self_history(packed):
    query, keys, values, valid = packed
    score_scale = HD ** (-0.5)
    scores = jnp.einsum('ihe,jhe->hij', query.astype(jnp.float32), keys.astype(jnp.float32)) * score_scale
    positions = jnp.arange(LENGTH, dtype=jnp.int32)
    allowed = (positions[None, :] <= positions[:, None]) & (positions[None, :] < valid)
    weights = jnp.where(allowed[None], jax.nn.silu(scores), 0.0).astype(jnp.bfloat16)
    result = jnp.einsum('hij,jhe->ihe', weights.astype(jnp.float32), values.astype(jnp.float32))
    return result.astype(jnp.bfloat16).reshape(LENGTH, D)

def reference(history, candidates, lengths, assignment, weight_in, weight_out, gain_in, gain_attn):
    score_scale = HD ** (-0.5)
    hist_float = history.astype(jnp.float32)
    normed = rms_apply(hist_float, gain_in).astype(jnp.bfloat16).reshape(HISTS * LENGTH, D)
    projected = jnp.dot(normed, weight_in, preferred_element_type=jnp.float32)
    gate = jax.nn.silu(projected[:, :D]).astype(jnp.bfloat16)
    query = projected[:, D:2 * D].astype(jnp.bfloat16).reshape(HISTS, LENGTH, H, HD)
    keys = projected[:, 2 * D:3 * D].astype(jnp.bfloat16).reshape(HISTS, LENGTH, H, HD)
    values = projected[:, 3 * D:].astype(jnp.bfloat16).reshape(HISTS, LENGTH, H, HD)
    attended = lax.map(self_history, (query, keys, values, lengths))
    attended = attended.reshape(HISTS * LENGTH, D).astype(jnp.float32)
    gated_rows = (rms_apply(attended, gain_attn) * gate.astype(jnp.float32)).astype(jnp.bfloat16)
    history_out = (hist_float.reshape(HISTS * LENGTH, D) + jnp.dot(gated_rows, weight_out, preferred_element_type=jnp.float32)).astype(jnp.bfloat16)
    history_out = history_out.reshape(HISTS, LENGTH, D)
    cand_float = candidates.astype(jnp.float32)
    cand_normed = rms_apply(cand_float, gain_in).astype(jnp.bfloat16).reshape(N_DP * CS, D)
    cand_proj = jnp.dot(cand_normed, weight_in[:, :2 * D], preferred_element_type=jnp.float32)
    cand_gate = jax.nn.silu(cand_proj[:, :D]).astype(jnp.bfloat16)
    cand_query = cand_proj[:, D:].astype(jnp.bfloat16).reshape(N_DP, CS, H, HD)
    block_rows = math.gcd(CS, 1024)
    positions = jnp.arange(LENGTH, dtype=jnp.int32)
    outputs = []
    for dp_index in range(N_DP):
        keys_here = keys[dp_index * HIST_DP:(dp_index + 1) * HIST_DP].astype(jnp.float32)
        values_here = values[dp_index * HIST_DP:(dp_index + 1) * HIST_DP].astype(jnp.float32)
        lengths_here = lengths[dp_index * HIST_DP:(dp_index + 1) * HIST_DP]

        def cross_block(packed):
            query_block, owner = packed
            summed = jnp.zeros((block_rows, H, HD), jnp.float32)
            for member in range(HIST_DP):
                scores = jnp.einsum('che,jhe->chj', query_block.astype(jnp.float32), keys_here[member]) * score_scale
                allowed = (positions[None, None, :] < lengths_here[member]) & (owner[:, None, None] == member)
                weights = jnp.where(allowed, jax.nn.silu(scores), 0.0).astype(jnp.bfloat16)
                summed = summed + jnp.einsum('chj,jhe->che', weights.astype(jnp.float32), values_here[member])
            return summed.astype(jnp.bfloat16)
        blocks = lax.map(cross_block, (cand_query[dp_index].reshape(CS // block_rows, block_rows, H, HD), assignment[dp_index].reshape(CS // block_rows, block_rows)))
        outputs.append(blocks.reshape(CS, D))
    cross_attended = jnp.stack(outputs).reshape(N_DP * CS, D).astype(jnp.float32)
    cand_gated = (rms_apply(cross_attended, gain_attn) * cand_gate.astype(jnp.float32)).astype(jnp.bfloat16)
    candidate_out = (cand_float.reshape(N_DP * CS, D) + jnp.dot(cand_gated, weight_out, preferred_element_type=jnp.float32)).astype(jnp.bfloat16)
    return (history_out, candidate_out.reshape(N_DP, CS, D))
```

```python
import functools

import jax
import jax.numpy as jnp
from jax import lax
from jax.experimental import pallas as pl
from jax.experimental.pallas import tpu as pltpu
from jax.sharding import PartitionSpec as P

H = 16
HD = 64
PAIR = 2 * HD
EPS = 1e-06
MESH = pl.DeviceIdType.MESH


def normed_rows(rows, gain):
    rows = rows.astype(jnp.float32)
    mean = jnp.mean(rows * rows, axis=-1, keepdims=True)
    return rows * lax.rsqrt(mean + EPS) * gain


def layer_kernel(
    ring,
    hist_hbm,
    cand_hbm,
    len_ref,
    assign_ref,
    w_in_hbm,
    w_out_hbm,
    gain_in_ref,
    gain_attn_ref,
    hist_out,
    cand_out,
    slots,
    own,
    cand,
    w_in,
    w_out,
    xn,
    gate,
    qz,
    kv,
    acc,
    lim,
    mask,
    load_sem,
    send_sem,
    recv_sem,
):
    hist_local, tok, width = own.shape
    cands = cand.shape[0]
    rows = tok + cands
    pairs = width // PAIR
    hist_rows = hist_local * tok
    half = ring // 2
    me = lax.axis_index("seq")
    right, left = lax.rem(me + 1, ring), lax.rem(me + ring - 1, ring)
    towards = (right, left)

    def send(src, slot, member, way):
        number = hist_local * slot + member
        return pltpu.make_async_remote_copy(
            src_ref=src,
            dst_ref=slots.at[slot, member, way],
            send_sem=send_sem.at[way, number],
            recv_sem=recv_sem.at[way, number],
            device_id={"seq": towards[way]},
            device_id_type=MESH,
        )

    loads = (
        pltpu.make_async_copy(hist_hbm, own, load_sem.at[0]),
        pltpu.make_async_copy(cand_hbm, cand, load_sem.at[1]),
        pltpu.make_async_copy(w_in_hbm, w_in, load_sem.at[2]),
        pltpu.make_async_copy(w_out_hbm, w_out, load_sem.at[3]),
    )
    for load in loads:
        load.start()

    barrier = pltpu.get_barrier_semaphore()
    for neighbour in towards:
        pl.semaphore_signal(barrier, inc=1, device_id={"seq": neighbour}, device_id_type=MESH)
    pl.semaphore_wait(barrier, 2)
    for member in range(hist_local):
        for way in range(2):
            send(hist_hbm.at[member], 0, member, way).start()

    gain_in = gain_in_ref[...]

    row_of = lax.broadcasted_iota(jnp.int32, (tok, 2 * PAIR), 0)
    eye = lax.broadcasted_iota(jnp.int32, (cands, cands), 0) == lax.broadcasted_iota(
        jnp.int32, (cands, cands), 1
    )
    owner = jnp.sum(
        jnp.where(eye, jnp.broadcast_to(assign_ref[...].astype(jnp.float32), (cands, cands)), 0.0),
        axis=1,
        keepdims=True,
    )
    for member in range(hist_local):
        valid = len_ref[member]
        lim[member, :tok, :] = jnp.minimum(me * tok + row_of + 1, valid).astype(jnp.float32)
        mine = jnp.where(owner == float(member), 1.0, 0.0)
        lim[member, tok:, :] = jnp.broadcast_to(mine, (cands, 2 * PAIR)) * valid.astype(jnp.float32)

    for load in loads[:3]:
        load.wait()
    for member in range(hist_local):
        xn[member * tok : (member + 1) * tok, :] = normed_rows(own[member], gain_in).astype(
            jnp.bfloat16
        )
    xn[hist_rows:, :] = normed_rows(cand[...], gain_in).astype(jnp.bfloat16)
    lane = lax.broadcasted_iota(jnp.int32, (1, PAIR), 1)
    first_head = lane < HD
    for block in range(width // 256):
        cols = slice(block * 256, (block + 1) * 256)
        part = 0.5 * jnp.dot(xn[...], w_in[:, cols], preferred_element_type=jnp.float32)
        gate[:, cols] = (part * (1.0 + jnp.tanh(part))).astype(jnp.bfloat16)
    for block in range(width // 256):
        cols = slice(width + block * 256, width + (block + 1) * 256)
        query = jnp.dot(xn[...], w_in[:, cols], preferred_element_type=jnp.float32)
        query = query.astype(jnp.bfloat16).astype(jnp.float32) * (0.5 * HD ** (-0.5))
        for inner in range(2):
            two = query[:, inner * PAIR : (inner + 1) * PAIR]
            for head in range(2):
                keep = jnp.where(first_head == (head == 0), two, 0.0).astype(jnp.bfloat16)
                for member in range(hist_local):
                    at = head * rows
                    qz[member, 2 * block + inner, at : at + tok, :] = keep[
                        member * tok : (member + 1) * tok
                    ]
                    qz[member, 2 * block + inner, at + tok : at + rows, :] = keep[hist_rows:]

    def project_keys():
        for block in range(2 * width // 256):
            start = 2 * width + block * 256
            part = jnp.dot(
                xn[:hist_rows, :], w_in[:, start : start + 256], preferred_element_type=jnp.float32
            ).astype(jnp.bfloat16)
            kv[2 * block] = part[:, :PAIR]
            kv[2 * block + 1] = part[:, PAIR:]

    def attend(member, key_rows, count, positions, fresh):
        mask[:, :count] = jnp.where(positions < lim[member, :, :count], 1.0, 0.0)
        for pair in range(pairs):
            half_score = lax.dot_general(
                qz[member, pair],
                kv[pair, key_rows, :],
                (((1,), (1,)), ((), ())),
                preferred_element_type=jnp.float32,
            )
            weights = []
            for head in range(2):
                part = half_score[head * rows : (head + 1) * rows]
                weights.append(
                    (part * mask[:, :count] * (1.0 + jnp.tanh(part))).astype(jnp.bfloat16)
                )
            values = kv[pairs + pair, key_rows, :]
            first = jnp.dot(weights[0], values, preferred_element_type=jnp.float32)
            second = jnp.dot(weights[1], values, preferred_element_type=jnp.float32)
            both = jnp.where(first_head, first, second)
            if fresh:
                acc[member, pair] = both
            else:
                acc[member, pair] += both

    def place_of(block, count):
        inside = lax.broadcasted_iota(jnp.int32, (1, count), 1)
        return (block * tok + inside).astype(jnp.float32)

    project_keys()
    for member in range(hist_local):
        attend(member, slice(member * tok, (member + 1) * tok), tok, place_of(me, tok), True)

    @pl.loop(0, hist_local * (half - 1))
    def _(number):
        step, member = number // hist_local, lax.rem(number, hist_local)
        for way in range(2):
            send(slots.at[step, member, way], step, member, way).wait_recv()

            @pl.when((step < half - 2) | (member == way))
            def _():
                send(slots.at[step, member, way], step + 1, member, way).start()

        for way in range(2):
            xn[way * tok : (way + 1) * tok, :] = normed_rows(
                slots[step, member, way], gain_in
            ).astype(jnp.bfloat16)
        project_keys()
        from_left = lax.rem(me + ring - 1 - step, ring)
        from_right = lax.rem(me + 1 + step, ring)
        inside = lax.broadcasted_iota(jnp.int32, (1, 2 * tok), 1)
        positions = jnp.where(
            inside < tok, from_left * tok + inside, (from_right - 1) * tok + inside
        ).astype(jnp.float32)
        attend(member, slice(0, 2 * tok), 2 * tok, positions, False)

    opposite = lax.rem(me + half, ring)
    for member in range(hist_local):
        send(slots.at[half - 1, member, member], half - 1, member, member).wait_recv()
        xn[member * tok : (member + 1) * tok, :] = normed_rows(
            slots[half - 1, member, member], gain_in
        ).astype(jnp.bfloat16)
    project_keys()
    for member in range(hist_local):
        attend(
            member, slice(member * tok, (member + 1) * tok), tok, place_of(opposite, tok), False
        )

    loads[3].wait()
    gain_attn = gain_attn_ref[...]

    def finish(attended, gates, residual):
        attended = attended.astype(jnp.bfloat16)
        gated = (normed_rows(attended, gain_attn) * gates.astype(jnp.float32)).astype(jnp.bfloat16)
        outs = jnp.dot(gated, w_out[...], preferred_element_type=jnp.float32)
        return (residual.astype(jnp.float32) + outs).astype(jnp.bfloat16)

    for member in range(hist_local):
        attended = jnp.concatenate([acc[member, pair, :tok, :] for pair in range(pairs)], axis=1)
        hist_out[member] = finish(
            attended, gate[member * tok : (member + 1) * tok, :], own[member]
        )
    crossed = jnp.concatenate(
        [
            sum(acc[member, pair, tok:, :] for member in range(hist_local))
            for pair in range(pairs)
        ],
        axis=1,
    )
    cand_out[...] = finish(crossed, gate[hist_rows:, :], cand[...])

    @pl.loop(0, hist_local * (half - 1))
    def _(number):
        step, member = number // hist_local, lax.rem(number, hist_local)
        for way in range(2):
            send(slots.at[step, member, way], step, member, way).wait_send()

    for member in range(hist_local):
        send(slots.at[half - 1, member, member], half - 1, member, member).wait_send()


def per_device(history, candidates, lengths, assignment, weight_in, weight_out, gain_in, gain_attn):
    ring = lax.axis_size("seq")
    hist_local, tok, width = history.shape
    cands = candidates.shape[1]
    rows = tok + cands
    pairs = width // PAIR
    half = ring // 2
    whole = pl.BlockSpec(memory_space=pltpu.VMEM)
    scalars = pl.BlockSpec(memory_space=pltpu.SMEM)
    there = pl.BlockSpec(memory_space=pl.ANY)
    history_out, candidate_out = pl.pallas_call(
        functools.partial(layer_kernel, ring),
        out_shape=(
            jax.ShapeDtypeStruct(history.shape, jnp.bfloat16),
            jax.ShapeDtypeStruct((cands, width), jnp.bfloat16),
        ),
        in_specs=[there, there, scalars, whole, there, there, whole, whole],
        out_specs=(whole, whole),
        scratch_shapes=[
            pltpu.VMEM((half, hist_local, 2, tok, width), jnp.bfloat16),
            pltpu.VMEM((hist_local, tok, width), jnp.bfloat16),
            pltpu.VMEM((cands, width), jnp.bfloat16),
            pltpu.VMEM(weight_in.shape, jnp.bfloat16),
            pltpu.VMEM(weight_out.shape, jnp.bfloat16),
            pltpu.VMEM((hist_local * tok + cands, width), jnp.bfloat16),
            pltpu.VMEM((hist_local * tok + cands, width), jnp.bfloat16),
            pltpu.VMEM((hist_local, pairs, 2 * rows, PAIR), jnp.bfloat16),
            pltpu.VMEM((2 * pairs, 2 * tok, PAIR), jnp.bfloat16),
            pltpu.VMEM((hist_local, pairs, rows, PAIR), jnp.float32),
            pltpu.VMEM((hist_local, rows, 2 * PAIR), jnp.float32),
            pltpu.VMEM((rows, 2 * PAIR), jnp.float32),
            pltpu.SemaphoreType.DMA((4,)),
            pltpu.SemaphoreType.DMA((2, hist_local * half)),
            pltpu.SemaphoreType.DMA((2, hist_local * half)),
        ],
        compiler_params=pltpu.CompilerParams(
            collective_id=0, has_side_effects=True, vmem_limit_bytes=60 * 1024 * 1024
        ),
    )(
        history,
        candidates[0],
        lengths,
        assignment,
        weight_in,
        weight_out,
        gain_in.reshape(1, width),
        gain_attn.reshape(1, width),
    )
    return history_out, candidate_out[None]


def solution(mesh):
    in_specs = (
        P(("groups", "dp"), "seq", None),
        P(("groups", "dp"), "seq", None),
        P(("groups", "dp")),
        P(("groups", "dp"), "seq"),
        P(),
        P(),
        P(),
        P(),
    )
    out_specs = (P(("groups", "dp"), "seq", None), P(("groups", "dp"), "seq", None))
    return jax.shard_map(
        per_device, mesh=mesh, in_specs=in_specs, out_specs=out_specs, check_vma=False
    )
```

```python
import functools

import jax
import jax.numpy as jnp
from jax import lax
from jax.experimental import pallas as pl
from jax.experimental.pallas import tpu as pltpu
from jax.sharding import PartitionSpec as P

HD = 64
PAIR = 2 * HD
EPS = 1e-06
MESH = pl.DeviceIdType.MESH
MOST_EXTRA = 2


def normed_rows(rows, gain):
    rows = rows.astype(jnp.float32)
    mean = jnp.mean(rows * rows, axis=-1, keepdims=True)
    return rows * lax.rsqrt(mean + EPS) * gain


def lead_of(place):
    return jnp.maximum(2 * MOST_EXTRA + 1 - place, 0) * jnp.minimum(place, 1)


def late_of(place):
    return MOST_EXTRA * jnp.maximum(1 - place, 0)


def extra_of(place):
    return lax.div(lead_of(place), 2) + late_of(place)


def attend_kernel(
    ring,
    hist_hbm,
    cand_hbm,
    len_ref,
    assign_ref,
    w_in_hbm,
    gain_in_ref,
    gain_attn_ref,
    gated_out,
    from_left,
    from_right,
    own,
    cand,
    w_in,
    xn,
    gate,
    qz,
    kv,
    acc,
    lim,
    mask,
    load_sem,
    right_send,
    right_recv,
    left_send,
    left_recv,
):
    hist_local, tok, width = own.shape
    cands = cand.shape[0]
    rows = tok + cands
    pairs = width // PAIR
    hist_rows = hist_local * tok
    base = ring - 1
    me = lax.axis_index("seq")
    right, left = lax.rem(me + 1, ring), lax.rem(me + ring - 1, ring)
    lead, late, extra = lead_of(me), late_of(me), extra_of(me)
    early = extra - late
    turns = base - extra
    count_right = base - extra_of(right)
    count_left = base + extra_of(left)

    def send_right(src, chunk):
        return pltpu.make_async_remote_copy(
            src_ref=src,
            dst_ref=from_left.at[chunk],
            send_sem=right_send.at[chunk],
            recv_sem=right_recv.at[chunk],
            device_id={"seq": right},
            device_id_type=MESH,
        )

    def send_left(src, chunk):
        return pltpu.make_async_remote_copy(
            src_ref=src,
            dst_ref=from_right.at[chunk],
            send_sem=left_send.at[chunk],
            recv_sem=left_recv.at[chunk],
            device_id={"seq": left},
            device_id_type=MESH,
        )

    def pass_right(chunk):
        send_right(from_left.at[chunk], chunk).wait_recv()

        @pl.when(chunk + 2 < count_right)
        def _():
            send_right(from_left.at[chunk], chunk + 2).start()

    def pass_left(chunk):
        send_left(from_right.at[chunk], chunk).wait_recv()

        @pl.when(chunk + 2 < count_left)
        def _():
            send_left(from_right.at[chunk], chunk + 2).start()

    barrier = pltpu.get_barrier_semaphore()
    for neighbour in (right, left):
        pl.semaphore_signal(barrier, inc=1, device_id={"seq": neighbour}, device_id_type=MESH)
    loads = (
        pltpu.make_async_copy(hist_hbm, own, load_sem.at[0]),
        pltpu.make_async_copy(cand_hbm, cand, load_sem.at[1]),
        pltpu.make_async_copy(w_in_hbm, w_in, load_sem.at[2]),
    )
    for load in loads:
        load.start()
    pl.semaphore_wait(barrier, 2)
    loads[0].wait()
    for chunk in range(hist_local):
        send_right(own.at[chunk], chunk).start()
        send_left(own.at[hist_local - 1 - chunk], chunk).start()

    gain_in = gain_in_ref[...]
    lane = lax.broadcasted_iota(jnp.int32, (1, PAIR), 1)
    first_head = lane < HD

    def project_keys():
        for block in range(2 * width // 256):
            start = 2 * width + block * 256
            part = jnp.dot(
                xn[:hist_rows, :], w_in[:, start : start + 256], preferred_element_type=jnp.float32
            ).astype(jnp.bfloat16)
            kv[2 * block] = part[:, :PAIR]
            kv[2 * block + 1] = part[:, PAIR:]

    def attend_rows(member, side, block, first_row, last_row, fresh):
        key_rows = slice(side * tok, (side + 1) * tok)
        count = last_row - first_row
        positions = block * tok + lax.broadcasted_iota(jnp.int32, (1, tok), 1)
        mask[first_row:last_row, :tok] = jnp.where(
            positions.astype(jnp.float32) < lim[member, first_row:last_row, :tok], 1.0, 0.0
        )
        for pair in range(pairs):
            half_score = lax.dot_general(
                qz[member, pair, 2 * first_row : 2 * last_row, :],
                kv[pair, key_rows, :],
                (((1,), (1,)), ((), ())),
                preferred_element_type=jnp.float32,
            )
            values = kv[pairs + pair, key_rows, :]
            parts = []
            for head in range(2):
                part = half_score[head * count : (head + 1) * count]
                weights = part * mask[first_row:last_row, :tok] * (1.0 + jnp.tanh(part))
                parts.append(
                    jnp.dot(
                        weights.astype(jnp.bfloat16), values, preferred_element_type=jnp.float32
                    )
                )
            both = jnp.where(first_head, parts[0], parts[1])
            if fresh:
                acc[member, pair, first_row:last_row, :] = both
            else:
                acc[member, pair, first_row:last_row, :] += both

    def attend(member, side, block):
        attend_rows(member, side, block, tok, rows, False)

        @pl.when(block < me)
        def _():
            attend_rows(member, side, block, 0, tok, False)

    row_of = lax.broadcasted_iota(jnp.int32, (tok, PAIR), 0)
    eye = lax.broadcasted_iota(jnp.int32, (cands, cands), 0) == lax.broadcasted_iota(
        jnp.int32, (cands, cands), 1
    )
    owners = jnp.broadcast_to(assign_ref[...].astype(jnp.float32), (cands, cands))
    owner = jnp.sum(jnp.where(eye, owners, 0.0), axis=1, keepdims=True)
    for member in range(hist_local):
        valid = len_ref[member]
        lim[member, :tok, :] = jnp.minimum(me * tok + row_of + 1, valid).astype(jnp.float32)
        mine = jnp.where(owner == float(member), 1.0, 0.0)
        lim[member, tok:, :] = jnp.broadcast_to(mine, (cands, PAIR)) * valid.astype(
            jnp.float32
        )

    for member in range(hist_local):
        xn[member * tok : (member + 1) * tok, :] = normed_rows(own[member], gain_in).astype(
            jnp.bfloat16
        )
    loads[1].wait()
    xn[hist_rows:, :] = normed_rows(cand[...], gain_in).astype(jnp.bfloat16)
    loads[2].wait()
    for block in range(width // 256):
        cols = slice(block * 256, (block + 1) * 256)
        part = 0.5 * jnp.dot(xn[...], w_in[:, cols], preferred_element_type=jnp.float32)
        gate[:, cols] = (part * (1.0 + jnp.tanh(part))).astype(jnp.bfloat16)
    for block in range(width // 256):
        cols = slice(width + block * 256, width + (block + 1) * 256)
        query = jnp.dot(xn[...], w_in[:, cols], preferred_element_type=jnp.float32)
        query = query.astype(jnp.bfloat16).astype(jnp.float32) * (0.5 * HD ** (-0.5))
        for inner in range(2):
            two = query[:, inner * PAIR : (inner + 1) * PAIR]
            for head in range(2):
                keep = jnp.where(first_head == (head == 0), two, 0.0).astype(jnp.bfloat16)
                for member in range(hist_local):
                    at = head * tok
                    qz[member, 2 * block + inner, at : at + tok, :] = keep[
                        member * tok : (member + 1) * tok
                    ]
                    at = 2 * tok + head * cands
                    qz[member, 2 * block + inner, at : at + cands, :] = keep[hist_rows:]
    project_keys()
    for member in range(hist_local):
        attend_rows(member, member, me, tok, rows, True)
        attend_rows(member, member, me, 0, tok, True)

    def unit(first, first_member, first_block, second, second_member, second_block):
        for side, chunk in enumerate((first, second)):
            xn[side * tok : (side + 1) * tok, :] = normed_rows(chunk[...], gain_in).astype(
                jnp.bfloat16
            )
        project_keys()
        attend(first_member, 0, first_block)
        attend(second_member, 1, second_block)

    def block_right(chunk):
        return lax.rem(me + 1 + lax.div(chunk, 2), ring)

    @pl.loop(0, lead)
    def _(chunk):
        pass_left(chunk)

    @pl.loop(0, turns)
    def _(turn):
        @pl.when(turn + lead < base + extra)
        def _():
            pass_left(turn + lead)

        pass_right(turn)
        other = turn + 2 * jnp.minimum(early, lax.div(jnp.maximum(turn - 1, 0), 2))
        member = lax.rem(turn, 2)
        unit(
            from_left.at[turn],
            member,
            lax.rem(me + ring - 1 - lax.div(turn, 2), ring),
            from_right.at[other],
            lax.rem(other + 1, 2),
            block_right(other),
        )

        due_late = (late > 0) & ((turn == turns - 4) | (turn == turns - 2))
        due_early = ((early > 0) & (turn == 2)) | ((early > 1) & (turn == 4))
        chunk = turn + 2 * late + (turn - 1) * jnp.minimum(me, 1)

        @pl.when(due_late)
        def _():
            pass_left(chunk)
            pass_left(chunk + 1)

        @pl.when(due_late | due_early)
        def _():
            unit(
                from_right.at[chunk],
                lax.rem(chunk + 1, 2),
                block_right(chunk),
                from_right.at[chunk + 1],
                lax.rem(chunk, 2),
                block_right(chunk + 1),
            )

    gain_attn = gain_attn_ref[...]

    def gated(attended, gates):
        attended = attended.astype(jnp.bfloat16)
        return (normed_rows(attended, gain_attn) * gates.astype(jnp.float32)).astype(jnp.bfloat16)

    for member in range(hist_local):
        mine = slice(member * tok, (member + 1) * tok)
        attended = jnp.concatenate([acc[member, pair, :tok, :] for pair in range(pairs)], axis=1)
        gated_out[mine, :] = gated(attended, gate[mine, :])
    crossed = jnp.concatenate(
        [
            sum(acc[member, pair, tok:, :] for member in range(hist_local))
            for pair in range(pairs)
        ],
        axis=1,
    )
    gated_out[hist_rows:, :] = gated(crossed, gate[hist_rows:, :])

    @pl.loop(0, count_right)
    def _(chunk):
        send_right(own.at[0], chunk).wait_send()

    @pl.loop(0, count_left)
    def _(chunk):
        send_left(own.at[0], chunk).wait_send()


def output_kernel(gated, w_out, history, candidates, history_out, candidate_out):
    hist_local, tok, width = history.shape
    hist_rows = hist_local * tok
    for block in range(width // 256):
        cols = slice(block * 256, (block + 1) * 256)
        outs = jnp.dot(gated[...], w_out[:, cols], preferred_element_type=jnp.float32)
        for member in range(hist_local):
            history_out[member, :, cols] = (
                history[member, :, cols].astype(jnp.float32)
                + outs[member * tok : (member + 1) * tok]
            ).astype(jnp.bfloat16)
        candidate_out[:, cols] = (
            candidates[:, cols].astype(jnp.float32) + outs[hist_rows:]
        ).astype(jnp.bfloat16)


def per_device(history, candidates, lengths, assignment, weight_in, weight_out, gain_in, gain_attn):
    ring = lax.axis_size("seq")
    hist_local, tok, width = history.shape
    cands = candidates.shape[1]
    rows = tok + cands
    all_rows = hist_local * tok + cands
    pairs = width // PAIR
    whole = pl.BlockSpec(memory_space=pltpu.VMEM)
    scalars = pl.BlockSpec(memory_space=pltpu.SMEM)
    there = pl.BlockSpec(memory_space=pltpu.HBM)
    gated = pl.pallas_call(
        functools.partial(attend_kernel, ring),
        out_shape=jax.ShapeDtypeStruct((all_rows, width), jnp.bfloat16),
        in_specs=[there, there, scalars, whole, there, whole, whole],
        out_specs=whole,
        scratch_shapes=[
            pltpu.VMEM((ring - 1, tok, width), jnp.bfloat16),
            pltpu.VMEM((ring - 1 + MOST_EXTRA, tok, width), jnp.bfloat16),
            pltpu.VMEM((hist_local, tok, width), jnp.bfloat16),
            pltpu.VMEM((cands, width), jnp.bfloat16),
            pltpu.VMEM(weight_in.shape, jnp.bfloat16),
            pltpu.VMEM((all_rows, width), jnp.bfloat16),
            pltpu.VMEM((all_rows, width), jnp.bfloat16),
            pltpu.VMEM((hist_local, pairs, 2 * rows, PAIR), jnp.bfloat16),
            pltpu.VMEM((2 * pairs, hist_local * tok, PAIR), jnp.bfloat16),
            pltpu.VMEM((hist_local, pairs, rows, PAIR), jnp.float32),
            pltpu.VMEM((hist_local, rows, PAIR), jnp.float32),
            pltpu.VMEM((rows, PAIR), jnp.float32),
            pltpu.SemaphoreType.DMA((3,)),
            pltpu.SemaphoreType.DMA((ring - 1,)),
            pltpu.SemaphoreType.DMA((ring - 1,)),
            pltpu.SemaphoreType.DMA((ring - 1 + MOST_EXTRA,)),
            pltpu.SemaphoreType.DMA((ring - 1 + MOST_EXTRA,)),
        ],
        compiler_params=pltpu.CompilerParams(
            collective_id=0, has_side_effects=True, vmem_limit_bytes=58 * 1024 * 1024
        ),
    )(
        history,
        candidates[0],
        lengths,
        assignment,
        weight_in,
        gain_in.reshape(1, width),
        gain_attn.reshape(1, width),
    )
    history_out, candidate_out = pl.pallas_call(
        output_kernel,
        out_shape=(
            jax.ShapeDtypeStruct(history.shape, jnp.bfloat16),
            jax.ShapeDtypeStruct((cands, width), jnp.bfloat16),
        ),
        in_specs=[whole, whole, whole, whole],
        out_specs=(whole, whole),
        compiler_params=pltpu.CompilerParams(vmem_limit_bytes=8 * 1024 * 1024),
    )(gated, weight_out, history, candidates[0])
    return history_out, candidate_out[None]


def solution(mesh):
    in_specs = (
        P(("groups", "dp"), "seq", None),
        P(("groups", "dp"), "seq", None),
        P(("groups", "dp")),
        P(("groups", "dp"), "seq"),
        P(),
        P(),
        P(),
        P(),
    )
    out_specs = (P(("groups", "dp"), "seq", None), P(("groups", "dp"), "seq", None))
    return jax.shard_map(
        per_device, mesh=mesh, in_specs=in_specs, out_specs=out_specs, check_vma=False
    )
```

```python
import functools

import jax
import jax.numpy as jnp
from jax import lax
from jax.experimental import pallas as pl
from jax.experimental.pallas import tpu as pltpu
from jax.sharding import PartitionSpec as P

HD = 64
PAIR = 2 * HD
EPS = 1e-06
MESH = pl.DeviceIdType.MESH
MOST_EXTRA = 2


def normed_rows(rows, gain):
    rows = rows.astype(jnp.float32)
    mean = jnp.mean(rows * rows, axis=-1, keepdims=True)
    return rows * lax.rsqrt(mean + EPS) * gain


def lead_of(place):
    return jnp.maximum(2 * MOST_EXTRA + 1 - place, 0) * jnp.minimum(place, 1)


def late_of(place):
    return MOST_EXTRA * jnp.maximum(1 - place, 0)


def back_of(place, ring):
    return jnp.maximum(place + 2 - ring, 0)


def extra_of(place, ring):
    return lax.div(lead_of(place), 2) + late_of(place) - back_of(place, ring)


def attend_kernel(
    ring,
    hist_hbm,
    cand_hbm,
    len_hbm,
    assign_hbm,
    w_in_hbm,
    gain_in_hbm,
    gain_attn_hbm,
    gated_hbm,
    slots,
    own,
    cand,
    len_ref,
    assign_ref,
    w_in,
    gain_in_ref,
    gain_attn_ref,
    gated_rows,
    xn,
    gate,
    qz,
    kv,
    acc,
    lim,
    mask,
    load_sem,
    store_sem,
    right_send,
    right_recv,
    left_send,
    left_recv,
):
    hist_local, tok, width = own.shape
    cands = cand.shape[0]
    rows = tok + cands
    pairs = width // PAIR
    hist_rows = hist_local * tok
    base = ring - 1
    me = lax.axis_index("seq")
    right, left = lax.rem(me + 1, ring), lax.rem(me + ring - 1, ring)
    lead, late, back, extra = lead_of(me), late_of(me), back_of(me, ring), extra_of(me, ring)
    early = lax.div(lead, 2)
    turns = base - early - late - back
    count_right = base - extra_of(right, ring)
    count_left = base + extra_of(left, ring)
    offset = base + MOST_EXTRA

    def send_right(src, chunk):
        return pltpu.make_async_remote_copy(
            src_ref=src,
            dst_ref=slots.at[chunk],
            send_sem=right_send.at[chunk],
            recv_sem=right_recv.at[chunk],
            device_id={"seq": right},
            device_id_type=MESH,
        )

    def send_left(src, chunk):
        return pltpu.make_async_remote_copy(
            src_ref=src,
            dst_ref=slots.at[offset + chunk],
            send_sem=left_send.at[chunk],
            recv_sem=left_recv.at[chunk],
            device_id={"seq": left},
            device_id_type=MESH,
        )

    def pass_right(chunk):
        send_right(slots.at[chunk], chunk).wait_recv()

        @pl.when(chunk + 2 < count_right)
        def _():
            send_right(slots.at[chunk], chunk + 2).start()

    def pass_left(chunk):
        send_left(slots.at[offset + chunk], chunk).wait_recv()

        @pl.when(chunk + 2 < count_left)
        def _():
            send_left(slots.at[offset + chunk], chunk + 2).start()

    barrier = pltpu.get_barrier_semaphore()
    for neighbour in (right, left):
        pl.semaphore_signal(barrier, inc=1, device_id={"seq": neighbour}, device_id_type=MESH)
    loads = (
        pltpu.make_async_copy(hist_hbm, own, load_sem.at[0]),
        pltpu.make_async_copy(cand_hbm, cand, load_sem.at[1]),
        pltpu.make_async_copy(gain_in_hbm, gain_in_ref, load_sem.at[2]),
        pltpu.make_async_copy(gain_attn_hbm, gain_attn_ref, load_sem.at[3]),
        pltpu.make_async_copy(len_hbm, len_ref, load_sem.at[4]),
        pltpu.make_async_copy(assign_hbm, assign_ref, load_sem.at[5]),
        pltpu.make_async_copy(w_in_hbm, w_in, load_sem.at[6]),
    )
    for load in loads:
        load.start()
    pl.semaphore_wait(barrier, 2)
    loads[0].wait()
    for chunk in range(hist_local):
        send_right(own.at[chunk], chunk).start()
        send_left(own.at[hist_local - 1 - chunk], chunk).start()

    for load in loads[1:6]:
        load.wait()
    gain_in = gain_in_ref[...]
    lane = lax.broadcasted_iota(jnp.int32, (1, PAIR), 1)
    first_head = lane < HD

    def project_keys():
        for block in range(2 * width // 256):
            start = 2 * width + block * 256
            part = jnp.dot(
                xn[:hist_rows, :], w_in[:, start : start + 256], preferred_element_type=jnp.float32
            ).astype(jnp.bfloat16)
            kv[2 * block] = part[:, :PAIR]
            kv[2 * block + 1] = part[:, PAIR:]

    def attend_rows(member, side, block, first_row, last_row, fresh):
        key_rows = slice(side * tok, (side + 1) * tok)
        count = last_row - first_row
        positions = block * tok + lax.broadcasted_iota(jnp.int32, (1, tok), 1)
        mask[first_row:last_row, :tok] = jnp.where(
            positions.astype(jnp.float32) < lim[member, first_row:last_row, :tok], 1.0, 0.0
        )
        for pair in range(pairs):
            half_score = lax.dot_general(
                qz[member, pair, 2 * first_row : 2 * last_row, :],
                kv[pair, key_rows, :],
                (((1,), (1,)), ((), ())),
                preferred_element_type=jnp.float32,
            )
            values = kv[pairs + pair, key_rows, :]
            parts = []
            for head in range(2):
                part = half_score[head * count : (head + 1) * count]
                weights = part * mask[first_row:last_row, :tok] * (1.0 + jnp.tanh(part))
                parts.append(
                    jnp.dot(
                        weights.astype(jnp.bfloat16), values, preferred_element_type=jnp.float32
                    )
                )
            both = jnp.where(first_head, parts[0], parts[1])
            if fresh:
                acc[member, pair, first_row:last_row, :] = both
            else:
                acc[member, pair, first_row:last_row, :] += both

    def attend(member, side, block):
        attend_rows(member, side, block, tok, rows, False)

        @pl.when(block < me)
        def _():
            attend_rows(member, side, block, 0, tok, False)

    row_of = lax.broadcasted_iota(jnp.int32, (tok, PAIR), 0)
    eye = lax.broadcasted_iota(jnp.int32, (cands, cands), 0) == lax.broadcasted_iota(
        jnp.int32, (cands, cands), 1
    )
    owners = jnp.broadcast_to(assign_ref[...].astype(jnp.float32), (cands, cands))
    owner = jnp.sum(jnp.where(eye, owners, 0.0), axis=1, keepdims=True)
    for member in range(hist_local):
        valid = len_ref[member]
        lim[member, :tok, :] = jnp.minimum(me * tok + row_of + 1, valid).astype(jnp.float32)
        mine = jnp.where(owner == float(member), 1.0, 0.0)
        lim[member, tok:, :] = jnp.broadcast_to(mine, (cands, PAIR)) * valid.astype(
            jnp.float32
        )

    for member in range(hist_local):
        xn[member * tok : (member + 1) * tok, :] = normed_rows(own[member], gain_in).astype(
            jnp.bfloat16
        )
    xn[hist_rows:, :] = normed_rows(cand[...], gain_in).astype(jnp.bfloat16)
    loads[6].wait()
    for block in range(width // 256):
        cols = slice(block * 256, (block + 1) * 256)
        part = 0.5 * jnp.dot(xn[...], w_in[:, cols], preferred_element_type=jnp.float32)
        gate[:, cols] = (part * (1.0 + jnp.tanh(part))).astype(jnp.bfloat16)
    for block in range(width // 256):
        cols = slice(width + block * 256, width + (block + 1) * 256)
        query = jnp.dot(xn[...], w_in[:, cols], preferred_element_type=jnp.float32)
        query = query.astype(jnp.bfloat16).astype(jnp.float32) * (0.5 * HD ** (-0.5))
        for inner in range(2):
            two = query[:, inner * PAIR : (inner + 1) * PAIR]
            for head in range(2):
                keep = jnp.where(first_head == (head == 0), two, 0.0).astype(jnp.bfloat16)
                for member in range(hist_local):
                    at = head * tok
                    qz[member, 2 * block + inner, at : at + tok, :] = keep[
                        member * tok : (member + 1) * tok
                    ]
                    at = 2 * tok + head * cands
                    qz[member, 2 * block + inner, at : at + cands, :] = keep[hist_rows:]
    project_keys()
    for member in range(hist_local):
        attend_rows(member, member, me, tok, rows, True)
        attend_rows(member, member, me, 0, tok, True)

    def unit(first, first_member, first_block, second, second_member, second_block):
        for side, slot in enumerate((first, second)):
            xn[side * tok : (side + 1) * tok, :] = normed_rows(slots[slot], gain_in).astype(
                jnp.bfloat16
            )
        project_keys()
        attend(first_member, 0, first_block)
        attend(second_member, 1, second_block)

    def block_at(way, chunk):
        return lax.rem(me + ring + way * (1 + lax.div(chunk, 2)), ring)

    @pl.loop(0, lead)
    def _(chunk):
        pass_left(chunk)

    @pl.loop(0, turns)
    def _(turn):
        @pl.when((turn + lead < base + extra) & ((late == 0) | (turn < turns - 2)))
        def _():
            pass_left(turn + lead)

        pass_right(turn)
        other = turn + 2 * jnp.minimum(early, lax.div(jnp.maximum(turn - 1, 0), 2))
        member = lax.rem(turn, 2)
        unit(
            turn,
            member,
            block_at(-1, turn),
            offset + other,
            lax.rem(other + 1, 2),
            block_at(1, other),
        )

        due_first, due_last = (late > 0) & (turn == turns - 3), (late > 0) & (turn == turns - 2)
        due_early = ((early > 0) & (turn == 2)) | ((early > 1) & (turn == 4))
        due_back = (back > 0) & (turn == turns - 1)
        chunk = 2 * turn - 1 + (7 - turns) * (1 - jnp.minimum(me, 1))
        chunk = (1 - back) * chunk + back * (turn + 1)

        @pl.when(due_first)
        def _():
            for ahead in range(1, 5):
                pass_left(turn + ahead)

        @pl.when(due_last)
        def _():
            for ahead in range(4, 6):
                pass_left(turn + ahead)

        @pl.when(due_back)
        def _():
            for ahead in range(1, 3):
                pass_right(turn + ahead)

        @pl.when(due_first | due_last | due_early | due_back)
        def _():
            slot = chunk + offset * (1 - back)
            unit(
                slot,
                lax.rem(chunk + 1 - back, 2),
                block_at(1 - 2 * back, chunk),
                slot + 1,
                lax.rem(chunk + back, 2),
                block_at(1 - 2 * back, chunk + 1),
            )

    gain_attn = gain_attn_ref[...]

    def gated(attended, gates):
        attended = attended.astype(jnp.bfloat16)
        return (normed_rows(attended, gain_attn) * gates.astype(jnp.float32)).astype(jnp.bfloat16)

    def store(first_row, last_row, number):
        there = pl.ds(first_row, last_row - first_row)
        return pltpu.make_async_copy(
            gated_rows.at[there], gated_hbm.at[there], store_sem.at[number]
        )

    stores = []
    for member in range(hist_local):
        mine = slice(member * tok, (member + 1) * tok)
        attended = jnp.concatenate([acc[member, pair, :tok, :] for pair in range(pairs)], axis=1)
        gated_rows[mine, :] = gated(attended, gate[mine, :])
        stores.append(store(mine.start, mine.stop, member))
        stores[-1].start()
    crossed = jnp.concatenate(
        [
            sum(acc[member, pair, tok:, :] for member in range(hist_local))
            for pair in range(pairs)
        ],
        axis=1,
    )
    gated_rows[hist_rows:, :] = gated(crossed, gate[hist_rows:, :])
    stores.append(store(hist_rows, hist_rows + cands, hist_local))
    stores[-1].start()

    @pl.loop(0, count_right)
    def _(chunk):
        send_right(own.at[0], chunk).wait_send()

    @pl.loop(0, count_left)
    def _(chunk):
        send_left(own.at[0], chunk).wait_send()

    for copy in stores:
        copy.wait()


def output_kernel(gated, w_out, history, candidates, history_out, candidate_out):
    hist_local, tok, width = history.shape
    hist_rows = hist_local * tok
    for block in range(width // 256):
        cols = slice(block * 256, (block + 1) * 256)
        outs = jnp.dot(gated[...], w_out[:, cols], preferred_element_type=jnp.float32)
        for member in range(hist_local):
            history_out[member, :, cols] = (
                history[member, :, cols].astype(jnp.float32)
                + outs[member * tok : (member + 1) * tok]
            ).astype(jnp.bfloat16)
        candidate_out[:, cols] = (
            candidates[:, cols].astype(jnp.float32) + outs[hist_rows:]
        ).astype(jnp.bfloat16)


def per_device(history, candidates, lengths, assignment, weight_in, weight_out, gain_in, gain_attn):
    ring = lax.axis_size("seq")
    hist_local, tok, width = history.shape
    cands = candidates.shape[1]
    rows = tok + cands
    all_rows = hist_local * tok + cands
    pairs = width // PAIR
    whole = pl.BlockSpec(memory_space=pltpu.VMEM)
    there = pl.BlockSpec(memory_space=pltpu.HBM)
    gated = pl.pallas_call(
        functools.partial(attend_kernel, ring),
        out_shape=jax.ShapeDtypeStruct((all_rows, width), jnp.bfloat16),
        in_specs=[there] * 7,
        out_specs=there,
        scratch_shapes=[
            pltpu.VMEM((2 * (ring - 1 + MOST_EXTRA), tok, width), jnp.bfloat16),
            pltpu.VMEM((hist_local, tok, width), jnp.bfloat16),
            pltpu.VMEM((cands, width), jnp.bfloat16),
            pltpu.SMEM(lengths.shape, jnp.int32),
            pltpu.VMEM(assignment.shape, jnp.int32),
            pltpu.VMEM(weight_in.shape, jnp.bfloat16),
            pltpu.VMEM((1, width), jnp.float32),
            pltpu.VMEM((1, width), jnp.float32),
            pltpu.VMEM((all_rows, width), jnp.bfloat16),
            pltpu.VMEM((all_rows, width), jnp.bfloat16),
            pltpu.VMEM((all_rows, width), jnp.bfloat16),
            pltpu.VMEM((hist_local, pairs, 2 * rows, PAIR), jnp.bfloat16),
            pltpu.VMEM((2 * pairs, hist_local * tok, PAIR), jnp.bfloat16),
            pltpu.VMEM((hist_local, pairs, rows, PAIR), jnp.float32),
            pltpu.VMEM((hist_local, rows, PAIR), jnp.float32),
            pltpu.VMEM((rows, PAIR), jnp.float32),
            pltpu.SemaphoreType.DMA((7,)),
            pltpu.SemaphoreType.DMA((hist_local + 1,)),
            pltpu.SemaphoreType.DMA((ring - 1 + MOST_EXTRA,)),
            pltpu.SemaphoreType.DMA((ring - 1 + MOST_EXTRA,)),
            pltpu.SemaphoreType.DMA((ring - 1 + MOST_EXTRA,)),
            pltpu.SemaphoreType.DMA((ring - 1 + MOST_EXTRA,)),
        ],
        compiler_params=pltpu.CompilerParams(
            collective_id=0, has_side_effects=True, vmem_limit_bytes=58 * 1024 * 1024
        ),
    )(
        history,
        candidates[0],
        lengths,
        assignment,
        weight_in,
        gain_in.reshape(1, width),
        gain_attn.reshape(1, width),
    )
    history_out, candidate_out = pl.pallas_call(
        output_kernel,
        out_shape=(
            jax.ShapeDtypeStruct(history.shape, jnp.bfloat16),
            jax.ShapeDtypeStruct((cands, width), jnp.bfloat16),
        ),
        in_specs=[whole, whole, whole, whole],
        out_specs=(whole, whole),
        compiler_params=pltpu.CompilerParams(vmem_limit_bytes=8 * 1024 * 1024),
    )(gated, weight_out, history, candidates[0])
    return history_out, candidate_out[None]


def solution(mesh):
    in_specs = (
        P(("groups", "dp"), "seq", None),
        P(("groups", "dp"), "seq", None),
        P(("groups", "dp")),
        P(("groups", "dp"), "seq"),
        P(),
        P(),
        P(),
        P(),
    )
    out_specs = (P(("groups", "dp"), "seq", None), P(("groups", "dp"), "seq", None))
    return jax.shard_map(
        per_device, mesh=mesh, in_specs=in_specs, out_specs=out_specs, check_vma=False
    )
```

```python
import functools

import jax
import jax.numpy as jnp
from jax import lax
from jax.experimental import pallas as pl
from jax.experimental.pallas import tpu as pltpu
from jax.sharding import PartitionSpec as P

HD = 64
PAIR = 2 * HD
EPS = 1e-06
MESH = pl.DeviceIdType.MESH
MOST_EXTRA = 2


def normed_rows(rows, gain):
    rows = rows.astype(jnp.float32)
    mean = jnp.mean(rows * rows, axis=-1, keepdims=True)
    return rows * lax.rsqrt(mean + EPS) * gain


def lead_of(place):
    return jnp.maximum(2 * MOST_EXTRA + 1 - place, 0) * jnp.minimum(place, 1)


def late_of(place):
    return MOST_EXTRA * jnp.maximum(1 - place, 0)


def back_of(place, ring):
    return jnp.maximum(place + 2 - ring, 0)


def extra_of(place, ring):
    return lax.div(lead_of(place), 2) + late_of(place) - back_of(place, ring)


def attend_kernel(
    ring,
    hist_hbm,
    cand_hbm,
    len_hbm,
    assign_hbm,
    w_in_hbm,
    gain_in_hbm,
    gain_attn_hbm,
    gated_out,
    slots,
    own,
    cand,
    len_ref,
    assign_ref,
    w_in,
    gain_in_ref,
    gain_attn_ref,
    xn,
    gate,
    qz,
    kv,
    acc,
    lim,
    mask,
    load_sem,
    right_send,
    right_recv,
    left_send,
    left_recv,
):
    hist_local, tok, width = own.shape
    cands = cand.shape[0]
    rows = tok + cands
    pairs = width // PAIR
    hist_rows = hist_local * tok
    base = ring - 1
    me = lax.axis_index("seq")
    right, left = lax.rem(me + 1, ring), lax.rem(me + ring - 1, ring)
    lead, late, back, extra = lead_of(me), late_of(me), back_of(me, ring), extra_of(me, ring)
    early = lax.div(lead, 2)
    turns = base - early - late - back
    count_right = base - extra_of(right, ring)
    count_left = base + extra_of(left, ring)
    offset = base + MOST_EXTRA

    def send_right(src, chunk):
        return pltpu.make_async_remote_copy(
            src_ref=src,
            dst_ref=slots.at[chunk],
            send_sem=right_send.at[chunk],
            recv_sem=right_recv.at[chunk],
            device_id={"seq": right},
            device_id_type=MESH,
        )

    def send_left(src, chunk):
        return pltpu.make_async_remote_copy(
            src_ref=src,
            dst_ref=slots.at[offset + chunk],
            send_sem=left_send.at[chunk],
            recv_sem=left_recv.at[chunk],
            device_id={"seq": left},
            device_id_type=MESH,
        )

    def pass_right(chunk):
        send_right(slots.at[chunk], chunk).wait_recv()

        @pl.when(chunk + 2 < count_right)
        def _():
            send_right(slots.at[chunk], chunk + 2).start()

    def pass_left(chunk):
        send_left(slots.at[offset + chunk], chunk).wait_recv()

        @pl.when(chunk + 2 < count_left)
        def _():
            send_left(slots.at[offset + chunk], chunk + 2).start()

    barrier = pltpu.get_barrier_semaphore()
    for neighbour in (right, left):
        pl.semaphore_signal(barrier, inc=1, device_id={"seq": neighbour}, device_id_type=MESH)
    loads = (
        pltpu.make_async_copy(hist_hbm, own, load_sem.at[0]),
        pltpu.make_async_copy(cand_hbm, cand, load_sem.at[1]),
        pltpu.make_async_copy(gain_in_hbm, gain_in_ref, load_sem.at[2]),
        pltpu.make_async_copy(gain_attn_hbm, gain_attn_ref, load_sem.at[3]),
        pltpu.make_async_copy(len_hbm, len_ref, load_sem.at[4]),
        pltpu.make_async_copy(assign_hbm, assign_ref, load_sem.at[5]),
        pltpu.make_async_copy(w_in_hbm, w_in, load_sem.at[6]),
    )
    for load in loads:
        load.start()
    pl.semaphore_wait(barrier, 2)
    loads[0].wait()
    for chunk in range(hist_local):
        send_right(own.at[chunk], chunk).start()
        send_left(own.at[hist_local - 1 - chunk], chunk).start()

    for load in loads[1:6]:
        load.wait()
    gain_in = gain_in_ref[...]
    lane = lax.broadcasted_iota(jnp.int32, (1, PAIR), 1)
    first_head = lane < HD

    def project_keys():
        for block in range(2 * width // 256):
            start = 2 * width + block * 256
            part = jnp.dot(
                xn[:hist_rows, :], w_in[:, start : start + 256], preferred_element_type=jnp.float32
            ).astype(jnp.bfloat16)
            kv[2 * block] = part[:, :PAIR]
            kv[2 * block + 1] = part[:, PAIR:]

    def attend_rows(member, side, block, first_row, last_row, fresh):
        key_rows = slice(side * tok, (side + 1) * tok)
        count = last_row - first_row
        positions = block * tok + lax.broadcasted_iota(jnp.int32, (1, tok), 1)
        mask[first_row:last_row, :tok] = jnp.where(
            positions.astype(jnp.float32) < lim[member, first_row:last_row, :tok], 1.0, 0.0
        )
        for pair in range(pairs):
            half_score = lax.dot_general(
                qz[member, pair, 2 * first_row : 2 * last_row, :],
                kv[pair, key_rows, :],
                (((1,), (1,)), ((), ())),
                preferred_element_type=jnp.float32,
            )
            values = kv[pairs + pair, key_rows, :]
            parts = []
            for head in range(2):
                part = half_score[head * count : (head + 1) * count]
                weights = part * mask[first_row:last_row, :tok] * (1.0 + jnp.tanh(part))
                parts.append(
                    jnp.dot(
                        weights.astype(jnp.bfloat16), values, preferred_element_type=jnp.float32
                    )
                )
            both = jnp.where(first_head, parts[0], parts[1])
            if fresh:
                acc[member, pair, first_row:last_row, :] = both
            else:
                acc[member, pair, first_row:last_row, :] += both

    def attend(member, side, block):
        attend_rows(member, side, block, tok, rows, False)

        @pl.when(block < me)
        def _():
            attend_rows(member, side, block, 0, tok, False)

    row_of = lax.broadcasted_iota(jnp.int32, (tok, PAIR), 0)
    eye = lax.broadcasted_iota(jnp.int32, (cands, cands), 0) == lax.broadcasted_iota(
        jnp.int32, (cands, cands), 1
    )
    owners = jnp.broadcast_to(assign_ref[...].astype(jnp.float32), (cands, cands))
    owner = jnp.sum(jnp.where(eye, owners, 0.0), axis=1, keepdims=True)
    for member in range(hist_local):
        valid = len_ref[member]
        lim[member, :tok, :] = jnp.minimum(me * tok + row_of + 1, valid).astype(jnp.float32)
        mine = jnp.where(owner == float(member), 1.0, 0.0)
        lim[member, tok:, :] = jnp.broadcast_to(mine, (cands, PAIR)) * valid.astype(
            jnp.float32
        )

    for member in range(hist_local):
        xn[member * tok : (member + 1) * tok, :] = normed_rows(own[member], gain_in).astype(
            jnp.bfloat16
        )
    xn[hist_rows:, :] = normed_rows(cand[...], gain_in).astype(jnp.bfloat16)
    loads[6].wait()
    for block in range(width // 256):
        cols = slice(block * 256, (block + 1) * 256)
        part = 0.5 * jnp.dot(xn[...], w_in[:, cols], preferred_element_type=jnp.float32)
        gate[:, cols] = (part * (1.0 + jnp.tanh(part))).astype(jnp.bfloat16)
    for block in range(width // 256):
        cols = slice(width + block * 256, width + (block + 1) * 256)
        query = jnp.dot(xn[...], w_in[:, cols], preferred_element_type=jnp.float32)
        query = query.astype(jnp.bfloat16).astype(jnp.float32) * (0.5 * HD ** (-0.5))
        for inner in range(2):
            two = query[:, inner * PAIR : (inner + 1) * PAIR]
            for head in range(2):
                keep = jnp.where(first_head == (head == 0), two, 0.0).astype(jnp.bfloat16)
                for member in range(hist_local):
                    at = head * tok
                    qz[member, 2 * block + inner, at : at + tok, :] = keep[
                        member * tok : (member + 1) * tok
                    ]
                    at = 2 * tok + head * cands
                    qz[member, 2 * block + inner, at : at + cands, :] = keep[hist_rows:]
    project_keys()
    for member in range(hist_local):
        attend_rows(member, member, me, tok, rows, True)
        attend_rows(member, member, me, 0, tok, True)

    def unit(first, first_member, first_block, second, second_member, second_block):
        for side, slot in enumerate((first, second)):
            xn[side * tok : (side + 1) * tok, :] = normed_rows(slots[slot], gain_in).astype(
                jnp.bfloat16
            )
        project_keys()
        attend(first_member, 0, first_block)
        attend(second_member, 1, second_block)

    def block_at(way, chunk):
        return lax.rem(me + ring + way * (1 + lax.div(chunk, 2)), ring)

    @pl.loop(0, lead)
    def _(chunk):
        pass_left(chunk)

    @pl.loop(0, turns)
    def _(turn):
        @pl.when((turn + lead < base + extra) & ((late == 0) | (turn < turns - 2)))
        def _():
            pass_left(turn + lead)

        pass_right(turn)
        other = turn + 2 * jnp.minimum(early, lax.div(jnp.maximum(turn - 1, 0), 2))
        member = lax.rem(turn, 2)
        unit(
            turn,
            member,
            block_at(-1, turn),
            offset + other,
            lax.rem(other + 1, 2),
            block_at(1, other),
        )

        due_first, due_last = (late > 0) & (turn == turns - 3), (late > 0) & (turn == turns - 2)
        due_early = ((early > 0) & (turn == 2)) | ((early > 1) & (turn == 4))
        due_back = (back > 0) & (turn == turns - 1)
        chunk = 2 * turn - 1 + (7 - turns) * (1 - jnp.minimum(me, 1))
        chunk = (1 - back) * chunk + back * (turn + 1)

        @pl.when(due_first)
        def _():
            for ahead in range(1, 5):
                pass_left(turn + ahead)

        @pl.when(due_last)
        def _():
            for ahead in range(4, 6):
                pass_left(turn + ahead)

        @pl.when(due_back)
        def _():
            for ahead in range(1, 3):
                pass_right(turn + ahead)

        @pl.when(due_first | due_last | due_early | due_back)
        def _():
            slot = chunk + offset * (1 - back)
            unit(
                slot,
                lax.rem(chunk + 1 - back, 2),
                block_at(1 - 2 * back, chunk),
                slot + 1,
                lax.rem(chunk + back, 2),
                block_at(1 - 2 * back, chunk + 1),
            )

    gain_attn = gain_attn_ref[...]

    def gated(attended, gates):
        attended = attended.astype(jnp.bfloat16)
        return (normed_rows(attended, gain_attn) * gates.astype(jnp.float32)).astype(jnp.bfloat16)

    for member in range(hist_local):
        mine = slice(member * tok, (member + 1) * tok)
        attended = jnp.concatenate([acc[member, pair, :tok, :] for pair in range(pairs)], axis=1)
        gated_out[mine, :] = gated(attended, gate[mine, :])
    crossed = jnp.concatenate(
        [
            sum(acc[member, pair, tok:, :] for member in range(hist_local))
            for pair in range(pairs)
        ],
        axis=1,
    )
    gated_out[hist_rows:, :] = gated(crossed, gate[hist_rows:, :])

    @pl.loop(0, count_right)
    def _(chunk):
        send_right(own.at[0], chunk).wait_send()

    @pl.loop(0, count_left)
    def _(chunk):
        send_left(own.at[0], chunk).wait_send()


def output_kernel(gated, w_out, history, candidates, history_out, candidate_out):
    hist_local, tok, width = history.shape
    hist_rows = hist_local * tok
    for block in range(width // 256):
        cols = slice(block * 256, (block + 1) * 256)
        outs = jnp.dot(gated[...], w_out[:, cols], preferred_element_type=jnp.float32)
        for member in range(hist_local):
            history_out[member, :, cols] = (
                history[member, :, cols].astype(jnp.float32)
                + outs[member * tok : (member + 1) * tok]
            ).astype(jnp.bfloat16)
        candidate_out[:, cols] = (
            candidates[:, cols].astype(jnp.float32) + outs[hist_rows:]
        ).astype(jnp.bfloat16)


def per_device(history, candidates, lengths, assignment, weight_in, weight_out, gain_in, gain_attn):
    ring = lax.axis_size("seq")
    hist_local, tok, width = history.shape
    cands = candidates.shape[1]
    rows = tok + cands
    all_rows = hist_local * tok + cands
    pairs = width // PAIR
    whole = pl.BlockSpec(memory_space=pltpu.VMEM)
    there = pl.BlockSpec(memory_space=pltpu.HBM)
    gated = pl.pallas_call(
        functools.partial(attend_kernel, ring),
        out_shape=pltpu.VMEM((all_rows, width), jnp.bfloat16),
        in_specs=[there] * 7,
        out_specs=whole,
        scratch_shapes=[
            pltpu.VMEM((2 * (ring - 1 + MOST_EXTRA), tok, width), jnp.bfloat16),
            pltpu.VMEM((hist_local, tok, width), jnp.bfloat16),
            pltpu.VMEM((cands, width), jnp.bfloat16),
            pltpu.SMEM(lengths.shape, jnp.int32),
            pltpu.VMEM(assignment.shape, jnp.int32),
            pltpu.VMEM(weight_in.shape, jnp.bfloat16),
            pltpu.VMEM((1, width), jnp.float32),
            pltpu.VMEM((1, width), jnp.float32),
            pltpu.VMEM((all_rows, width), jnp.bfloat16),
            pltpu.VMEM((all_rows, width), jnp.bfloat16),
            pltpu.VMEM((hist_local, pairs, 2 * rows, PAIR), jnp.bfloat16),
            pltpu.VMEM((2 * pairs, hist_local * tok, PAIR), jnp.bfloat16),
            pltpu.VMEM((hist_local, pairs, rows, PAIR), jnp.float32),
            pltpu.VMEM((hist_local, rows, PAIR), jnp.float32),
            pltpu.VMEM((rows, PAIR), jnp.float32),
            pltpu.SemaphoreType.DMA((7,)),
            pltpu.SemaphoreType.DMA((ring - 1 + MOST_EXTRA,)),
            pltpu.SemaphoreType.DMA((ring - 1 + MOST_EXTRA,)),
            pltpu.SemaphoreType.DMA((ring - 1 + MOST_EXTRA,)),
            pltpu.SemaphoreType.DMA((ring - 1 + MOST_EXTRA,)),
        ],
        compiler_params=pltpu.CompilerParams(
            collective_id=0, has_side_effects=True, vmem_limit_bytes=58 * 1024 * 1024
        ),
    )(
        history,
        candidates[0],
        lengths,
        assignment,
        weight_in,
        gain_in.reshape(1, width),
        gain_attn.reshape(1, width),
    )
    history_out, candidate_out = pl.pallas_call(
        output_kernel,
        out_shape=(
            jax.ShapeDtypeStruct(history.shape, jnp.bfloat16),
            jax.ShapeDtypeStruct((cands, width), jnp.bfloat16),
        ),
        in_specs=[whole, whole, whole, whole],
        out_specs=(whole, whole),
        compiler_params=pltpu.CompilerParams(vmem_limit_bytes=8 * 1024 * 1024),
    )(gated, weight_out, history, candidates[0])
    return history_out, candidate_out[None]


def solution(mesh):
    in_specs = (
        P(("groups", "dp"), "seq", None),
        P(("groups", "dp"), "seq", None),
        P(("groups", "dp")),
        P(("groups", "dp"), "seq"),
        P(),
        P(),
        P(),
        P(),
    )
    out_specs = (P(("groups", "dp"), "seq", None), P(("groups", "dp"), "seq", None))
    return jax.shard_map(
        per_device, mesh=mesh, in_specs=in_specs, out_specs=out_specs, check_vma=False
    )
```

```python
import functools

import jax
import jax.numpy as jnp
from jax import lax
from jax.experimental import pallas as pl
from jax.experimental.pallas import tpu as pltpu
from jax.sharding import PartitionSpec as P

HD = 64
PAIR = 2 * HD
EPS = 1e-06
MESH = pl.DeviceIdType.MESH
MOST_EXTRA = 2


def normed_rows(rows, gain):
    rows = rows.astype(jnp.float32)
    mean = jnp.mean(rows * rows, axis=-1, keepdims=True)
    return rows * lax.rsqrt(mean + EPS) * gain


def lead_of(place):
    return jnp.maximum(2 * MOST_EXTRA + 1 - place, 0) * jnp.minimum(place, 1)


def late_of(place):
    return MOST_EXTRA * jnp.maximum(1 - place, 0)


def back_of(place, ring):
    return jnp.maximum(place + 2 - ring, 0)


def extra_of(place, ring):
    return lax.div(lead_of(place), 2) + late_of(place) - back_of(place, ring)


def attend_kernel(
    ring,
    hist_hbm,
    cand_hbm,
    len_hbm,
    assign_hbm,
    w_in_hbm,
    gain_in_hbm,
    gain_attn_hbm,
    gated_out,
    slots,
    own,
    cand,
    len_ref,
    assign_ref,
    w_in,
    gain_in_ref,
    gain_attn_ref,
    xn,
    gate,
    qz,
    kv,
    acc,
    lim,
    mask,
    load_sem,
    right_send,
    right_recv,
    left_send,
    left_recv,
):
    hist_local, tok, width = own.shape
    cands = cand.shape[0]
    rows = tok + cands
    pairs = width // PAIR
    hist_rows = hist_local * tok
    base = ring - 1
    me = lax.axis_index("seq")
    right, left = lax.rem(me + 1, ring), lax.rem(me + ring - 1, ring)
    lead, late, back, extra = lead_of(me), late_of(me), back_of(me, ring), extra_of(me, ring)
    early = lax.div(lead, 2)
    turns = base - early - late - back
    count_right = base - extra_of(right, ring)
    count_left = base + extra_of(left, ring)
    offset = base + MOST_EXTRA

    def send_right(src, chunk):
        return pltpu.make_async_remote_copy(
            src_ref=src,
            dst_ref=slots.at[chunk],
            send_sem=right_send.at[chunk],
            recv_sem=right_recv.at[chunk],
            device_id={"seq": right},
            device_id_type=MESH,
        )

    def send_left(src, chunk):
        return pltpu.make_async_remote_copy(
            src_ref=src,
            dst_ref=slots.at[offset + chunk],
            send_sem=left_send.at[chunk],
            recv_sem=left_recv.at[chunk],
            device_id={"seq": left},
            device_id_type=MESH,
        )

    def pass_right(chunk):
        send_right(slots.at[chunk], chunk).wait_recv()

        @pl.when(chunk + 2 < count_right)
        def _():
            send_right(slots.at[chunk], chunk + 2).start()

    def pass_left(chunk):
        send_left(slots.at[offset + chunk], chunk).wait_recv()

        @pl.when(chunk + 2 < count_left)
        def _():
            send_left(slots.at[offset + chunk], chunk + 2).start()

    barrier = pltpu.get_barrier_semaphore()
    for neighbour in (right, left):
        pl.semaphore_signal(barrier, inc=1, device_id={"seq": neighbour}, device_id_type=MESH)
    loads = (
        pltpu.make_async_copy(hist_hbm, own, load_sem.at[0]),
        pltpu.make_async_copy(cand_hbm, cand, load_sem.at[1]),
        pltpu.make_async_copy(gain_in_hbm, gain_in_ref, load_sem.at[2]),
        pltpu.make_async_copy(gain_attn_hbm, gain_attn_ref, load_sem.at[3]),
        pltpu.make_async_copy(len_hbm, len_ref, load_sem.at[4]),
        pltpu.make_async_copy(assign_hbm, assign_ref, load_sem.at[5]),
        pltpu.make_async_copy(w_in_hbm, w_in, load_sem.at[6]),
    )
    for load in loads[:6]:
        load.start()
    loads[0].wait()
    loads[6].start()
    pl.semaphore_wait(barrier, 2)
    for chunk in range(hist_local):
        send_right(own.at[chunk], chunk).start()
        send_left(own.at[hist_local - 1 - chunk], chunk).start()

    for load in loads[1:6]:
        load.wait()
    gain_in = gain_in_ref[...]
    lane = lax.broadcasted_iota(jnp.int32, (1, PAIR), 1)
    first_head = lane < HD

    def project_keys():
        for block in range(2 * width // 256):
            start = 2 * width + block * 256
            part = jnp.dot(
                xn[:hist_rows, :], w_in[:, start : start + 256], preferred_element_type=jnp.float32
            ).astype(jnp.bfloat16)
            kv[2 * block] = part[:, :PAIR]
            kv[2 * block + 1] = part[:, PAIR:]

    def attend_rows(member, side, block, first_row, last_row, fresh):
        key_rows = slice(side * tok, (side + 1) * tok)
        count = last_row - first_row
        positions = block * tok + lax.broadcasted_iota(jnp.int32, (1, tok), 1)
        mask[first_row:last_row, :tok] = jnp.where(
            positions.astype(jnp.float32) < lim[member, first_row:last_row, :tok], 1.0, 0.0
        )
        for pair in range(pairs):
            half_score = lax.dot_general(
                qz[member, pair, 2 * first_row : 2 * last_row, :],
                kv[pair, key_rows, :],
                (((1,), (1,)), ((), ())),
                preferred_element_type=jnp.float32,
            )
            values = kv[pairs + pair, key_rows, :]
            parts = []
            for head in range(2):
                part = half_score[head * count : (head + 1) * count]
                weights = part * mask[first_row:last_row, :tok] * (1.0 + jnp.tanh(part))
                parts.append(
                    jnp.dot(
                        weights.astype(jnp.bfloat16), values, preferred_element_type=jnp.float32
                    )
                )
            both = jnp.where(first_head, parts[0], parts[1])
            if fresh:
                acc[member, pair, first_row:last_row, :] = both
            else:
                acc[member, pair, first_row:last_row, :] += both

    def attend(member, side, block):
        attend_rows(member, side, block, tok, rows, False)

        @pl.when(block < me)
        def _():
            attend_rows(member, side, block, 0, tok, False)

    row_of = lax.broadcasted_iota(jnp.int32, (tok, PAIR), 0)
    eye = lax.broadcasted_iota(jnp.int32, (cands, cands), 0) == lax.broadcasted_iota(
        jnp.int32, (cands, cands), 1
    )
    owners = jnp.broadcast_to(assign_ref[...].astype(jnp.float32), (cands, cands))
    owner = jnp.sum(jnp.where(eye, owners, 0.0), axis=1, keepdims=True)
    for member in range(hist_local):
        valid = len_ref[member]
        lim[member, :tok, :] = jnp.minimum(me * tok + row_of + 1, valid).astype(jnp.float32)
        mine = jnp.where(owner == float(member), 1.0, 0.0)
        lim[member, tok:, :] = jnp.broadcast_to(mine, (cands, PAIR)) * valid.astype(
            jnp.float32
        )

    for member in range(hist_local):
        xn[member * tok : (member + 1) * tok, :] = normed_rows(own[member], gain_in).astype(
            jnp.bfloat16
        )
    xn[hist_rows:, :] = normed_rows(cand[...], gain_in).astype(jnp.bfloat16)
    loads[6].wait()
    for block in range(width // 256):
        cols = slice(block * 256, (block + 1) * 256)
        part = 0.5 * jnp.dot(xn[...], w_in[:, cols], preferred_element_type=jnp.float32)
        gate[:, cols] = (part * (1.0 + jnp.tanh(part))).astype(jnp.bfloat16)
    for block in range(width // 256):
        cols = slice(width + block * 256, width + (block + 1) * 256)
        query = jnp.dot(xn[...], w_in[:, cols], preferred_element_type=jnp.float32)
        query = query.astype(jnp.bfloat16).astype(jnp.float32) * (0.5 * HD ** (-0.5))
        for inner in range(2):
            two = query[:, inner * PAIR : (inner + 1) * PAIR]
            for head in range(2):
                keep = jnp.where(first_head == (head == 0), two, 0.0).astype(jnp.bfloat16)
                for member in range(hist_local):
                    at = head * tok
                    qz[member, 2 * block + inner, at : at + tok, :] = keep[
                        member * tok : (member + 1) * tok
                    ]
                    at = 2 * tok + head * cands
                    qz[member, 2 * block + inner, at : at + cands, :] = keep[hist_rows:]
    project_keys()
    for member in range(hist_local):
        attend_rows(member, member, me, tok, rows, True)
        attend_rows(member, member, me, 0, tok, True)

    def unit(first, first_member, first_block, second, second_member, second_block):
        for side, slot in enumerate((first, second)):
            xn[side * tok : (side + 1) * tok, :] = normed_rows(slots[slot], gain_in).astype(
                jnp.bfloat16
            )
        project_keys()
        attend(first_member, 0, first_block)
        attend(second_member, 1, second_block)

    def block_at(way, chunk):
        return lax.rem(me + ring + way * (1 + lax.div(chunk, 2)), ring)

    @pl.loop(0, lead)
    def _(chunk):
        pass_left(chunk)

    @pl.loop(0, turns)
    def _(turn):
        @pl.when((turn + lead < base + extra) & ((late == 0) | (turn < turns - 2)))
        def _():
            pass_left(turn + lead)

        pass_right(turn)
        other = turn + 2 * jnp.minimum(early, lax.div(jnp.maximum(turn - 1, 0), 2))
        member = lax.rem(turn, 2)
        unit(
            turn,
            member,
            block_at(-1, turn),
            offset + other,
            lax.rem(other + 1, 2),
            block_at(1, other),
        )

        due_first, due_last = (late > 0) & (turn == turns - 3), (late > 0) & (turn == turns - 2)
        due_early = ((early > 0) & (turn == 2)) | ((early > 1) & (turn == 4))
        due_back = (back > 0) & (turn == turns - 1)
        chunk = 2 * turn - 1 + (7 - turns) * (1 - jnp.minimum(me, 1))
        chunk = (1 - back) * chunk + back * (turn + 1)

        @pl.when(due_first)
        def _():
            for ahead in range(1, 5):
                pass_left(turn + ahead)

        @pl.when(due_last)
        def _():
            for ahead in range(4, 6):
                pass_left(turn + ahead)

        @pl.when(due_back)
        def _():
            for ahead in range(1, 3):
                pass_right(turn + ahead)

        @pl.when(due_first | due_last | due_early | due_back)
        def _():
            slot = chunk + offset * (1 - back)
            unit(
                slot,
                lax.rem(chunk + 1 - back, 2),
                block_at(1 - 2 * back, chunk),
                slot + 1,
                lax.rem(chunk + back, 2),
                block_at(1 - 2 * back, chunk + 1),
            )

    gain_attn = gain_attn_ref[...]

    def gated(attended, gates):
        attended = attended.astype(jnp.bfloat16)
        return (normed_rows(attended, gain_attn) * gates.astype(jnp.float32)).astype(jnp.bfloat16)

    for member in range(hist_local):
        mine = slice(member * tok, (member + 1) * tok)
        attended = jnp.concatenate([acc[member, pair, :tok, :] for pair in range(pairs)], axis=1)
        gated_out[mine, :] = gated(attended, gate[mine, :])
    crossed = jnp.concatenate(
        [
            sum(acc[member, pair, tok:, :] for member in range(hist_local))
            for pair in range(pairs)
        ],
        axis=1,
    )
    gated_out[hist_rows:, :] = gated(crossed, gate[hist_rows:, :])

    @pl.loop(0, count_right)
    def _(chunk):
        send_right(own.at[0], chunk).wait_send()

    @pl.loop(0, count_left)
    def _(chunk):
        send_left(own.at[0], chunk).wait_send()


def output_kernel(gated, w_out, history, candidates, history_out, candidate_out):
    hist_local, tok, width = history.shape
    hist_rows = hist_local * tok
    for block in range(width // 256):
        cols = slice(block * 256, (block + 1) * 256)
        outs = jnp.dot(gated[...], w_out[:, cols], preferred_element_type=jnp.float32)
        for member in range(hist_local):
            history_out[member, :, cols] = (
                history[member, :, cols].astype(jnp.float32)
                + outs[member * tok : (member + 1) * tok]
            ).astype(jnp.bfloat16)
        candidate_out[:, cols] = (
            candidates[:, cols].astype(jnp.float32) + outs[hist_rows:]
        ).astype(jnp.bfloat16)


def per_device(history, candidates, lengths, assignment, weight_in, weight_out, gain_in, gain_attn):
    ring = lax.axis_size("seq")
    hist_local, tok, width = history.shape
    cands = candidates.shape[1]
    rows = tok + cands
    all_rows = hist_local * tok + cands
    pairs = width // PAIR
    whole = pl.BlockSpec(memory_space=pltpu.VMEM)
    there = pl.BlockSpec(memory_space=pltpu.HBM)
    gated = pl.pallas_call(
        functools.partial(attend_kernel, ring),
        out_shape=pltpu.VMEM((all_rows, width), jnp.bfloat16),
        in_specs=[there] * 7,
        out_specs=whole,
        scratch_shapes=[
            pltpu.VMEM((2 * (ring - 1 + MOST_EXTRA), tok, width), jnp.bfloat16),
            pltpu.VMEM((hist_local, tok, width), jnp.bfloat16),
            pltpu.VMEM((cands, width), jnp.bfloat16),
            pltpu.SMEM(lengths.shape, jnp.int32),
            pltpu.VMEM(assignment.shape, jnp.int32),
            pltpu.VMEM(weight_in.shape, jnp.bfloat16),
            pltpu.VMEM((1, width), jnp.float32),
            pltpu.VMEM((1, width), jnp.float32),
            pltpu.VMEM((all_rows, width), jnp.bfloat16),
            pltpu.VMEM((all_rows, width), jnp.bfloat16),
            pltpu.VMEM((hist_local, pairs, 2 * rows, PAIR), jnp.bfloat16),
            pltpu.VMEM((2 * pairs, hist_local * tok, PAIR), jnp.bfloat16),
            pltpu.VMEM((hist_local, pairs, rows, PAIR), jnp.float32),
            pltpu.VMEM((hist_local, rows, PAIR), jnp.float32),
            pltpu.VMEM((rows, PAIR), jnp.float32),
            pltpu.SemaphoreType.DMA((7,)),
            pltpu.SemaphoreType.DMA((ring - 1 + MOST_EXTRA,)),
            pltpu.SemaphoreType.DMA((ring - 1 + MOST_EXTRA,)),
            pltpu.SemaphoreType.DMA((ring - 1 + MOST_EXTRA,)),
            pltpu.SemaphoreType.DMA((ring - 1 + MOST_EXTRA,)),
        ],
        compiler_params=pltpu.CompilerParams(
            collective_id=0, has_side_effects=True, vmem_limit_bytes=58 * 1024 * 1024
        ),
    )(
        history,
        candidates[0],
        lengths,
        assignment,
        weight_in,
        gain_in.reshape(1, width),
        gain_attn.reshape(1, width),
    )
    history_out, candidate_out = pl.pallas_call(
        output_kernel,
        out_shape=(
            jax.ShapeDtypeStruct(history.shape, jnp.bfloat16),
            jax.ShapeDtypeStruct((cands, width), jnp.bfloat16),
        ),
        in_specs=[whole, whole, whole, whole],
        out_specs=(whole, whole),
        compiler_params=pltpu.CompilerParams(vmem_limit_bytes=8 * 1024 * 1024),
    )(gated, weight_out, history, candidates[0])
    return history_out, candidate_out[None]


def solution(mesh):
    in_specs = (
        P(("groups", "dp"), "seq", None),
        P(("groups", "dp"), "seq", None),
        P(("groups", "dp")),
        P(("groups", "dp"), "seq"),
        P(),
        P(),
        P(),
        P(),
    )
    out_specs = (P(("groups", "dp"), "seq", None), P(("groups", "dp"), "seq", None))
    return jax.shard_map(
        per_device, mesh=mesh, in_specs=in_specs, out_specs=out_specs, check_vma=False
    )
```
